32 devices in a mesh: row: 2 (over y), col: 16 (over z, x, core).
Axes of the slice: x: 2, y: 2, z: 4, core: 2. Of those that a mesh axis runs over, the one named last changes fastest.
Arguments:
- queries: bfloat16 [4096, 128], P(('row', 'col')), may hold values from -8 to 8
- key_rows: bfloat16 [4096, 128], P(('row', 'col')), may hold values from -8 to 8
- value_rows: bfloat16 [4096, 128], P(('row', 'col')), may hold values from -6 to 6
- grad_output: bfloat16 [4096, 128], P(('row', 'col')), may hold values from -6 to 6
- positions: int32 [4096], replicated, may hold values from 0 to 4095, as said below
Outputs:
- grad_queries: bfloat16 [4096, 128], P(('row', 'col'))
- grad_keys: bfloat16 [4096, 128], P(('row', 'col'))
- grad_values: bfloat16 [4096, 128], P(('row', 'col'))
The draws below stay inside these ranges and needn't reach their ends.
Inputs may be any that keep to these rules, and one draw needn't show every extreme that they name: `positions`: a permutation: each of 0 to 4095 appears once.
All inputs are finite; a program needn't handle non-finite values.
Results may differ from the reference program's by a relative error of at most 0.0068.
Values may be sent and summed in bfloat16 or wider, within the bound.
No kernel may reach another device: no remote copies, remote signals or barrier semaphores. Data moves between devices by JAX's collectives and lax.ppermute only.
A program may use at most 128 MiB of HBM per device.

```python
import math
import jax
import jax.numpy as jnp
from jax import lax

D = 128
TOKENS = 4096


def make_positions(key):
    return jax.random.permutation(jax.random.fold_in(key, 11), TOKENS).astype(jnp.int32)


def draw_positions(key, part):
    return make_positions(key)


def draw_queries(key, part):
    base = jax.random.normal(jax.random.fold_in(key, 21), (TOKENS, D), jnp.float32)
    return jnp.clip(base, -8.0, 8.0).astype(jnp.bfloat16)


def draw_key_rows(key, part):
    base = jax.random.normal(jax.random.fold_in(key, 22), (TOKENS, D), jnp.float32)
    return jnp.clip(base, -8.0, 8.0).astype(jnp.bfloat16)


def block_scale(own_key, shape, cuts, smallest, largest):
    def one(axis_at, blocks):
        steps = jax.random.uniform(jax.random.fold_in(jax.random.fold_in(own_key, 6), axis_at), (blocks,), jnp.float32, smallest / len(cuts), largest / len(cuts))
        return jnp.repeat(jnp.exp(steps), shape[axis_at] // blocks).reshape((-1,) + (1,) * (len(shape) - axis_at - 1))

    gain = one(*cuts[0])
    for cut in cuts[1:]:
        gain = gain * one(*cut)
    return gain


def normal_values(key, extent, width, limit, pieces=(), kind=jnp.bfloat16):
    entries = width * jax.random.normal(key, extent, jnp.float32)
    if pieces:
        entries = entries * block_scale(key, extent, pieces, -0.22, 0.18)
    return jnp.clip(entries, -limit, limit).astype(kind)


def setup_inputs(seed: int = 0) -> dict:
    seeds = jax.random.split(jax.random.key(seed), 6)
    return {
        "queries": draw_queries(jax.random.fold_in(seeds[5], 71), 0),
        "key_rows": draw_key_rows(jax.random.fold_in(seeds[5], 71), 0),
        "value_rows": normal_values(seeds[2], (TOKENS, D), 1.0, 6.0, ((0, 32),)),
        "grad_output": normal_values(seeds[3], (TOKENS, D), 1.0, 6.0, ((0, 32),)),
        "positions": draw_positions(jax.random.fold_in(seeds[5], 71), 0),
    }


def reference(queries, key_rows, value_rows, grad_output, positions):
    score_scale = 1.0 / math.sqrt(D)
    block_rows = 1024 if TOKENS % 1024 == 0 else TOKENS
    blocks_total = TOKENS // block_rows

    def query_block_step(state_pair, which):
        grad_keys, grad_values = state_pair
        begin_row = (which * block_rows).astype(jnp.int32)
        query_block = lax.dynamic_slice_in_dim(queries, begin_row, block_rows, 0)
        grad_block = lax.dynamic_slice_in_dim(grad_output, begin_row, block_rows, 0)
        query_order = lax.dynamic_slice_in_dim(positions, begin_row, block_rows, 0)
        scores = jnp.dot(query_block, key_rows.T, preferred_element_type=jnp.float32) * score_scale
        allowed = query_order[:, None] >= positions[None, :]
        run_max = lax.optimization_barrier(jnp.max(jnp.where(allowed, scores, -1e+30), axis=1, keepdims=True))
        run_sum = lax.optimization_barrier(jnp.sum(jnp.where(allowed, jnp.exp(scores - run_max), 0.0), axis=1, keepdims=True))
        log_total = run_max + jnp.log(run_sum)
        probs = jnp.where(allowed, jnp.exp(scores - log_total), 0.0)
        dprobs = jnp.dot(grad_block, value_rows.T, preferred_element_type=jnp.float32)
        delta = lax.optimization_barrier(jnp.sum(probs * dprobs, axis=1, keepdims=True))
        dscores = (probs * (dprobs - delta)).astype(jnp.bfloat16)
        probs_low = probs.astype(jnp.bfloat16)
        grad_query = jnp.dot(dscores, key_rows, preferred_element_type=jnp.float32) * score_scale
        grad_keys = grad_keys + jnp.dot(dscores.T, query_block, preferred_element_type=jnp.float32) * score_scale
        grad_values = grad_values + jnp.dot(probs_low.T, grad_block, preferred_element_type=jnp.float32)
        return ((grad_keys, grad_values), grad_query)
    zeros_pair = (jnp.zeros((TOKENS, D), jnp.float32), jnp.zeros((TOKENS, D), jnp.float32))
    (grad_keys, grad_values), grad_queries = lax.scan(query_block_step, zeros_pair, jnp.arange(blocks_total, dtype=jnp.int32))
    grad_queries = grad_queries.reshape(TOKENS, D)
    return (grad_queries.astype(jnp.bfloat16), grad_keys.astype(jnp.bfloat16), grad_values.astype(jnp.bfloat16))
```

```python
import math

import jax
import jax.numpy as jnp
from jax import lax
from jax.experimental import pallas as pl
from jax.experimental.pallas import tpu as pltpu
from jax.sharding import PartitionSpec as P


AXES = ("row", "col")
MASKED = -1e30
LOG2E = math.log2(math.e)
VMEM = pl.BlockSpec(memory_space=pltpu.VMEM)
SMEM = pl.BlockSpec(memory_space=pltpu.SMEM)
NT = (((1,), (1,)), ((), ()))
TN = (((0,), (0,)), ((), ()))


def dot(a, b, dims=(((1,), (0,)), ((), ()))):
    return lax.dot_general(a, b, dims, preferred_element_type=jnp.float32)


def subsets(bits):
    masks = [0]
    for bit in bits:
        masks = masks + [m | (1 << bit) for m in masks]
    return masks


def over(count, unroll, step):
    if unroll:
        for i in range(count):
            step(i)
    else:

        @pl.loop(0, count)
        def _(i):
            step(i)


def key_columns(idx, pos, first, count, t):
    return [
        jnp.transpose(jnp.broadcast_to(pos[pl.ds(idx[first + b], 1), :], (t, t)))
        for b in range(count)
    ]


def query_refs(qd0, qd1, i, half, t):
    def at(ref, j):
        return ref.at[pl.ds(j * t, t), :]

    return at(qd0, i) if i < half else at(qd1, i - half)


def make_stats(t, d, slots, blocks, scale):
    unroll = slots * blocks <= 64
    half = slots // 2

    def kernel(idx, pos, qd0, qd1, *rest):
        kvs, out = rest[:blocks], rest[blocks]
        columns = key_columns(idx, pos, slots, blocks, t)

        def side(ref, base):
            def step(i):
                query_pos = pos[pl.ds(idx[base + i], 1), :]
                start = i * t if unroll else pl.multiple_of(i * t, t)
                rows = ref[pl.ds(start, t), :]
                parts = []
                for b in range(blocks):
                    kv = kvs[b][...]
                    s = dot(kv[:, :d], rows[:, :d], NT)
                    dp = dot(kv[:, d:], rows[:, d:], NT)
                    s = jnp.where(query_pos >= columns[b], s, MASKED)
                    top = jnp.max(s, axis=0, keepdims=True)
                    e = jnp.exp2((s - top) * (scale * LOG2E))
                    parts.append(
                        (top, jnp.sum(e, 0, keepdims=True), jnp.sum(e * dp, 0, keepdims=True))
                    )
                m, l, o = combine(parts, scale)
                lanes = pl.ds(base * t + start, t)
                out[0:1, lanes] = m
                out[1:2, lanes] = l
                out[2:3, lanes] = o

            over(half, unroll, step)

        side(qd0, 0)
        side(qd1, half)

    return pl.pallas_call(
        kernel,
        in_specs=[SMEM] + [VMEM] * (3 + blocks),
        out_specs=VMEM,
        out_shape=jax.ShapeDtypeStruct((3, slots * t), jnp.float32),
        name="stats",
    )


def combine(parts, scale):
    m = parts[0][0]
    for p in parts[1:]:
        m = jnp.maximum(m, p[0])
    total = weighted = None
    for top, l, o in parts:
        w = jnp.exp2((top - m) * (scale * LOG2E))
        total = l * w if total is None else total + l * w
        weighted = o * w if weighted is None else weighted + o * w
    return m, total, weighted


def make_grads(t, d, slots, blocks, scale):
    unroll = slots * blocks <= 64
    half = slots // 2
    c = scale * LOG2E

    def kernel(idx, pos, qd0, qd1, *rest):
        kvs = rest[:blocks]
        sts = rest[blocks : blocks + half]
        dq_keep, dq_send = rest[blocks + half : blocks + half + 2]
        dkvs = rest[blocks + half + 2 : blocks + half + 2 + blocks]
        probs, dscores, shift, delta = rest[-4:]
        columns = key_columns(idx, pos, slots, blocks, t)

        for side in range(2):
            for j in range(half):
                at = (side * half + j) * t
                parts = []
                for k in range(half):
                    lanes = slice((side * half + (j ^ k)) * t, (side * half + (j ^ k) + 1) * t)
                    parts.append(tuple(sts[k][r : r + 1, lanes] for r in range(3)))
                m, l, o = combine(parts, scale)
                shift[0:1, at : at + t] = m * c + jnp.log2(l)
                delta[0:1, at : at + t] = o / l

        def side(ref, base):
            def step(i):
                query_pos = pos[pl.ds(idx[base + i], 1), :]
                start = i * t if unroll else pl.multiple_of(i * t, t)
                rows = ref[pl.ds(start, t), :]
                lanes = pl.ds(base * t + start, t)
                sh = shift[0:1, lanes]
                de = delta[0:1, lanes]
                for b in range(blocks):
                    kv = kvs[b][...]
                    s = dot(kv[:, :d], rows[:, :d], NT)
                    dp = dot(kv[:, d:], rows[:, d:], NT)
                    p = jnp.where(query_pos >= columns[b], jnp.exp2(s * c - sh), 0.0)
                    probs[b * t : (b + 1) * t, lanes] = p.astype(jnp.bfloat16)
                    dscores[b * t : (b + 1) * t, lanes] = (p * (dp - de)).astype(jnp.bfloat16)

            over(half, unroll, step)

        side(qd0, 0)
        side(qd1, half)

        q0, q1 = qd0[...], qd1[...]
        cut = half * t
        for b in range(blocks):
            rows = slice(b * t, (b + 1) * t)
            ds, pr = dscores[rows, :], probs[rows, :]
            dk = (dot(ds[:, :cut], q0[:, :d]) + dot(ds[:, cut:], q1[:, :d])) * scale
            dv = dot(pr[:, :cut], q0[:, d:]) + dot(pr[:, cut:], q1[:, d:])
            dkvs[b][:, :d] = dk.astype(dkvs[b].dtype)
            dkvs[b][:, d:] = dv.astype(dkvs[b].dtype)
        keys = jnp.concatenate([kv[:, :d] for kv in kvs], axis=0)
        for part, ref in ((slice(0, cut), dq_keep), (slice(cut, 2 * cut), dq_send)):
            dqt = dot(keys, dscores[:, part], TN) * scale
            ref[...] = jnp.transpose(dqt).astype(ref.dtype)

    f32, low = jnp.float32, jnp.bfloat16
    shape = jax.ShapeDtypeStruct
    return pl.pallas_call(
        kernel,
        in_specs=[SMEM] + [VMEM] * (3 + blocks + half),
        out_specs=[VMEM] * (2 + blocks),
        out_shape=[shape((half * t, d), f32), shape((half * t, d), f32), shape((t, 2 * d), f32)]
        + [shape((t, 2 * d), low)] * (blocks - 1),
        scratch_shapes=[
            pltpu.VMEM((blocks * t, slots * t), low),
            pltpu.VMEM((blocks * t, slots * t), low),
            pltpu.VMEM((1, slots * t), f32),
            pltpu.VMEM((1, slots * t), f32),
        ],
        name="grads",
    )


def body(queries, key_rows, value_rows, grad_output, positions):
    t, d = queries.shape
    scale = 1.0 / math.sqrt(d)
    rows, cols = lax.axis_size("row"), lax.axis_size("col")
    devices = rows * cols
    row_bits, col_bits = rows.bit_length() - 1, cols.bit_length() - 1
    assert devices == 1 << (row_bits + col_bits)
    key_masks = subsets(range(2, col_bits))
    query_masks = subsets([1] + list(range(col_bits, col_bits + row_bits)))
    half, blocks = len(query_masks), len(key_masks)
    slots = 2 * half
    me = lax.axis_index("row") * cols + lax.axis_index("col")

    def swap(a, mask):
        return lax.ppermute(a, AXES, [(i, i ^ mask) for i in range(devices)])

    masks = query_masks + [m ^ 1 for m in query_masks] + key_masks
    idx = me.astype(jnp.int32) ^ jnp.array(masks, jnp.int32)
    pos = positions.reshape(devices, t)

    kv = jnp.concatenate([key_rows, value_rows], axis=1)
    qd = jnp.concatenate([queries, grad_output], axis=1)
    kvs = [kv] + [swap(kv, m) for m in key_masks[:0:-1]][::-1]
    qd0 = jnp.concatenate([qd] + [swap(qd, m) for m in query_masks[1:]], axis=0)
    qd1 = swap(qd0, 1)

    own = make_stats(t, d, slots, blocks, scale)(idx, pos, qd0, qd1, *kvs)
    cut = half * t
    other = swap(own, 1)
    other = jnp.concatenate([other[:, cut:], other[:, :cut]], axis=1)
    both = jnp.concatenate(
        combine(
            [tuple(a[r : r + 1] for r in range(3)) for a in (own, other)],
            scale,
        ),
        axis=0,
    )
    sts = [both] + [swap(both, m) for m in query_masks[1:]]

    dq_keep, dq_send, dkv, *dkvs = make_grads(t, d, slots, blocks, scale)(
        idx, pos, qd0, qd1, *kvs, *sts
    )
    received = [swap(a, m) for a, m in zip(dkvs[::-1], key_masks[:0:-1])]
    dq = dq_keep + swap(dq_send, 1)
    dq_parts = [
        swap(dq[k * t : (k + 1) * t].astype(jnp.bfloat16), query_masks[k]) for k in range(1, half)
    ]
    grad_q = dq[:t]
    for part in dq_parts:
        grad_q = grad_q + part.astype(jnp.float32)
    for part in received:
        dkv = dkv + part.astype(jnp.float32)
    return (
        grad_q.astype(jnp.bfloat16),
        dkv[:, :d].astype(jnp.bfloat16),
        dkv[:, d:].astype(jnp.bfloat16),
    )


def solution(mesh):
    spec = P(AXES, None)
    return jax.shard_map(
        body,
        mesh=mesh,
        in_specs=(spec, spec, spec, spec, P()),
        out_specs=(spec, spec, spec),
        check_vma=False,
    )
```
